32 devices in a mesh: grid: 32 (over z, y, x, core).
Axes of the slice: x: 2, y: 2, z: 4, core: 2. Of those that a mesh axis runs over, the one named last changes fastest.
Arguments:
- right_sides: float32 [32, 32, 48, 128], P(None, 'grid'), may hold values from -54 to 54, as said below
- recycle: float32 [2, 24, 32, 48, 128], P(None, None, 'grid'), may hold values from -6 to 6
- medium: float32 [32, 48, 128], P('grid'), may hold values from 0.05 to 1
- shift_table: float32 [8], replicated, may hold values from 0.25 to 2
- shift_index: int32 [2], replicated, may hold values from 0 to 7
Outputs:
- solution: float32 [32, 32, 48, 128], P(None, 'grid')
- residue: float32 [32, 32, 48, 128], P(None, 'grid')
The draws below stay inside these ranges and needn't reach their ends.
Inputs may be any that keep to these rules, and one draw needn't show every extreme that they name: `right_sides`: finite real values.
All inputs are finite; a program needn't handle non-finite values.
Results may differ from the reference program's by a relative error of at most 0.0003.
Values sent between devices are 32-bit elements; how exact they have to be, the bound alone decides.
A program may use at most 64 MiB of HBM per device.

```python
import math
import jax
import jax.numpy as jnp
from jax import lax

NX = 48
NY = 128
K = 24
B = 16
STEPS = 3
SHIFTS = 8
S = 32
NZ = 32


def draw_right_sides(key, part):
    keys = jax.random.split(key, 3)
    plane = jnp.exp(jax.random.uniform(keys[1], (NZ,), jnp.float32, math.log(0.3), math.log(3.0)))
    rising = 0.5 + jnp.arange(NZ, dtype=jnp.float32) / max(NZ - 1, 1)
    column = jnp.exp(jax.random.uniform(keys[2], (S,), jnp.float32, math.log(0.3), math.log(3.0)))
    rough = jnp.clip(jax.random.normal(keys[0], (S, NZ, NX, NY), jnp.float32), -4.0, 4.0)
    return rough * column[:, None, None, None] * (plane * rising)[None, :, None, None]


def level_of(rng, shape, shards, low, high):
    factor_of, own = 1.0, jax.random.fold_in(rng, 6)
    for axis_at, blocks in shards:
        heights = jnp.exp(jax.random.uniform(jax.random.fold_in(own, axis_at), (blocks,), jnp.float32, low / len(shards), high / len(shards)))
        factor_of = factor_of * jnp.repeat(heights, shape[axis_at] // blocks).reshape([-1 if axis == axis_at else 1 for axis in range(len(shape))])
    return factor_of


def gaussian(key, shape, scale, most, cuts=(), kind=jnp.bfloat16):
    entries = scale * jax.random.normal(key, shape, jnp.float32)
    if cuts:
        entries = entries * level_of(key, shape, cuts, -0.22, 0.18)
    return jnp.clip(entries, -most, most).astype(kind)


def setup_inputs(seed: int = 0) -> dict:
    key_of = jax.random.split(jax.random.key(seed), 6)
    return {
        "right_sides": draw_right_sides(jax.random.fold_in(key_of[5], 71), 0),
        "recycle": gaussian(key_of[1], (2, K, NZ, NX, NY), 1.0, 6.0, ((2, 32),), jnp.float32),
        "medium": jnp.clip(jnp.exp(math.log(1.0) - 2.9957323 * jax.random.uniform(key_of[2], (NZ, NX, NY), jnp.float32) ** level_of(key_of[2], (NZ, NX, NY), ((0, 32),), -0.2, 0.2)), 0.05, 1.0),
        "shift_table": jnp.clip(jnp.exp(jax.random.uniform(key_of[3], (SHIFTS,), jnp.float32, math.log(0.25), math.log(2.0))), 0.25, 2.0),
        "shift_index": jax.random.randint(key_of[4], (2,), 0, SHIFTS).astype(jnp.int32),
    }


highest = lax.Precision.HIGHEST

def operate(field, diagonal_field):
    padded = jnp.pad(field, ((0, 0), (1, 1), (1, 1), (1, 1)))
    beside = padded[:, 2:, 1:-1, 1:-1] + padded[:, :-2, 1:-1, 1:-1]
    beside = beside + padded[:, 1:-1, 2:, 1:-1] + padded[:, 1:-1, :-2, 1:-1]
    beside = beside + padded[:, 1:-1, 1:-1, 2:] + padded[:, 1:-1, 1:-1, :-2]
    return diagonal_field * field - beside

def flat_rows(field):
    return field.reshape(field.shape[0], -1)

def gram_of(left, right):
    return jnp.dot(left, right.T, precision=highest)

def combine(coeffs, vectors):
    return jnp.dot(coeffs, vectors, precision=highest)

def lower_solve(factor, values):
    return jax.scipy.linalg.solve_triangular(factor, values, lower=True)

def upper_solve(factor, values):
    return jax.scipy.linalg.solve_triangular(factor, values, lower=True, trans=1)

def least_squares(hessenberg, target):
    normal_factor = jnp.linalg.cholesky(jnp.dot(hessenberg.T, hessenberg, precision=highest))
    right_part = jnp.dot(hessenberg.T, target, precision=highest)
    return upper_solve(normal_factor, lower_solve(normal_factor, right_part))

def reference(right_sides, recycle, medium, shift_table, shift_index):
    field_shape = right_sides.shape[1:]
    solutions = []
    residues = []
    for member in range(2):
        diagonal_field = 6.0 + shift_table[shift_index[member]] + medium
        sources = flat_rows(right_sides[member * B:(member + 1) * B])
        basis_u = recycle[member]
        applied_u = flat_rows(operate(basis_u, diagonal_field))
        factor = jnp.linalg.cholesky(gram_of(applied_u, applied_u))
        projected = lower_solve(factor, gram_of(applied_u, sources))
        residual = sources - combine(upper_solve(factor, projected).T, applied_u)
        resid_factor = jnp.linalg.cholesky(gram_of(residual, residual))
        blocks = [lower_solve(resid_factor, residual)]
        hess_cols = []
        recycle_cols = []
        for number in range(STEPS):
            applied = flat_rows(operate(blocks[number].reshape((B,) + field_shape), diagonal_field))
            recycle_part = lower_solve(factor, gram_of(applied_u, applied))
            krylov_parts = [gram_of(block, applied) for block in blocks]
            applied = applied - combine(upper_solve(factor, recycle_part).T, applied_u)
            for block, part in zip(blocks, krylov_parts):
                applied = applied - combine(part.T, block)
            new_factor = jnp.linalg.cholesky(gram_of(applied, applied))
            hess_cols.append(jnp.concatenate(krylov_parts + [new_factor.T, jnp.zeros(((STEPS - 1 - number) * B, B), jnp.float32)], axis=0))
            recycle_cols.append(recycle_part)
            blocks.append(lower_solve(new_factor, applied))
        hessenberg = jnp.concatenate(hess_cols, axis=1)
        recycle_coef = jnp.concatenate(recycle_cols, axis=1)
        target = jnp.concatenate([resid_factor.T, jnp.zeros((STEPS * B, B), jnp.float32)], axis=0)
        minimizer = least_squares(hessenberg, target)
        back_coef = upper_solve(factor, projected - combine(recycle_coef, minimizer))
        krylov = jnp.concatenate(blocks[:STEPS], axis=0)
        solution = combine(minimizer.T, krylov) + combine(back_coef.T, flat_rows(basis_u))
        residue = combine((target - combine(hessenberg, minimizer)).T, jnp.concatenate(blocks, axis=0))
        solutions.append(solution.reshape((B,) + field_shape))
        residues.append(residue.reshape((B,) + field_shape))
    return (jnp.concatenate(solutions, axis=0), jnp.concatenate(residues, axis=0))
```

```python
import functools

import jax
import jax.numpy as jnp
from jax import lax
from jax.experimental import pallas as pl
from jax.experimental.pallas import tpu as pltpu
from jax.sharding import PartitionSpec as P

STEPS = 3
LANES = 128
MESH = pl.DeviceIdType.MESH
highest = lax.Precision.HIGHEST


def dot(left, right):
    return lax.dot_general(
        left, right, (((1,), (0,)), ((), ())), precision=highest, preferred_element_type=jnp.float32
    )


def dot_t(left, right):
    return lax.dot_general(
        left, right, (((1,), (1,)), ((), ())), precision=highest, preferred_element_type=jnp.float32
    )


def iota2(shape, dim):
    return lax.broadcasted_iota(jnp.int32, shape, dim)


def eye(size):
    return jnp.where(iota2((size, size), 0) == iota2((size, size), 1), 1.0, 0.0)


def factor_all(matrices, count):
    size = matrices[0].shape[0]
    rows = iota2((size, 1), 0)
    unit = jnp.where(rows < count, eye(size), 0.0)
    parts = [(m, unit) for m in matrices]
    for k in range(count):
        fresh = []
        for a, z in parts:
            scale = 1.0 / a[k : k + 1, k : k + 1]
            f = jnp.where(rows > k, a[:, k : k + 1] * scale, 0.0)
            fresh.append((a - f * a[k : k + 1, :], z - f * z[k : k + 1, :]))
        parts = fresh
    upper = iota2((size, size), 1) >= iota2((size, size), 0)
    out = []
    for a, z in parts:
        pivots = jnp.sum(a * unit, axis=1, keepdims=True)
        root = jnp.where(rows < count, lax.rsqrt(jnp.where(rows < count, pivots, 1.0)), 0.0)
        out.append((jnp.where(upper, a * root, 0.0), z * root))
    return out


def solve_all(matrices, rights):
    size = matrices[0].shape[0]
    rows = iota2((size, 1), 0)
    unit = eye(size)
    parts = list(zip(matrices, rights))
    for k in range(size):
        fresh = []
        for a, r in parts:
            scale = 1.0 / a[k : k + 1, k : k + 1]
            f = jnp.where(rows == k, 0.0, a[:, k : k + 1] * scale)
            fresh.append((a - f * a[k : k + 1, :], r - f * r[k : k + 1, :]))
        parts = fresh
    return [r / jnp.sum(a * unit, axis=1, keepdims=True) for a, r in parts]


def kernel(
    n, factors, chunk,
    u_ref, b_ref, med_ref, table_ref, index_ref, sol_ref, res_ref,
    space, halo_u, halo_v, gram0, gram, coef, hbt, ebt, fin, back,
    send_sem, recv_sem, red_send, red_recv,
):
    me = lax.axis_index("grid")
    k_rows = u_ref.shape[1]
    block = b_ref.shape[1]
    cells = b_ref.shape[2]
    count = cells // chunk
    pad = space.shape[1] - (STEPS + 1) * block
    left, right = me - 1, me + 1
    has = (me > 0, me < n - 1)

    barrier = pltpu.get_barrier_semaphore()
    peers = []
    stride = 1
    for f in factors:
        mine = lax.rem(me // stride, f)
        base = me - mine * stride
        peers.append((f, stride, mine, base))
        stride *= f
    total = 0
    for f, stride, mine, base in peers:
        for d in range(1, f):
            pl.semaphore_signal(
                barrier, inc=1, device_id=(base + lax.rem(mine + d, f) * stride,), device_id_type=MESH
            )
            total += 1
    for to in (lax.rem(me + n - 1, n), lax.rem(me + 1, n)):
        pl.semaphore_signal(barrier, inc=1, device_id=(to,), device_id_type=MESH)
    pl.semaphore_wait(barrier, total + 2)

    def halo_copy(stage, side, i):
        inner = pl.ds(pl.multiple_of(i * chunk, LANES), chunk)
        outer = pl.ds(pl.multiple_of(i * chunk + LANES, LANES), chunk)
        if stage == 0:
            src, dst = u_ref.at[:, :, outer], halo_u.at[side, :, :, inner]
        else:
            src = space.at[:, pl.ds(pad + block * (stage - 1), block), outer]
            dst = halo_v.at[stage - 1, side, :, :, inner]
        return pltpu.make_async_remote_copy(
            src_ref=src, dst_ref=dst,
            send_sem=send_sem.at[stage, side, i], recv_sem=recv_sem.at[stage, side, i],
            device_id=((left, right)[side],), device_id_type=MESH,
        )

    def halo_start(stage, i):
        for side in range(2):
            @pl.when(has[side])
            def _():
                halo_copy(stage, side, i).start()

    def halo_wait(stage, i):
        for side in range(2):
            @pl.when(has[1 - side])
            def _():
                halo_copy(stage, side, i).wait_recv()

    def reduce_sum(buffer, number, values):
        offset = 0
        for f, stride, mine, base in peers:
            own = offset + mine
            for g in range(2):
                buffer[number, own, g, :, :] = values[g]
            for d in range(1, f):
                to = lax.rem(mine + d, f)
                pltpu.make_async_remote_copy(
                    src_ref=buffer.at[number, own], dst_ref=buffer.at[number, own],
                    send_sem=red_send.at[number if buffer is gram0 else number + 1, offset + d],
                    recv_sem=red_recv.at[number if buffer is gram0 else number + 1, own],
                    device_id=(base + to * stride,), device_id_type=MESH,
                ).start()
            for d in range(1, f):
                there = lax.rem(mine + d, f)
                origin = offset + there
                pltpu.make_async_remote_copy(
                    src_ref=buffer.at[number, origin], dst_ref=buffer.at[number, origin],
                    send_sem=red_send.at[number if buffer is gram0 else number + 1, offset + d],
                    recv_sem=red_recv.at[number if buffer is gram0 else number + 1, origin],
                    device_id=(base + there * stride,), device_id_type=MESH,
                ).wait_recv()
            values = []
            for g in range(2):
                value = buffer[number, offset, g, :, :]
                for s in range(1, f):
                    value = value + buffer[number, offset + s, g, :, :]
                values.append(value)
            offset += f
        return values

    def reduce_drain(buffer, number):
        offset = 0
        for f, stride, mine, base in peers:
            for d in range(1, f):
                pltpu.make_async_remote_copy(
                    src_ref=buffer.at[number, offset + mine], dst_ref=buffer.at[number, offset + mine],
                    send_sem=red_send.at[number if buffer is gram0 else number + 1, offset + d],
                    recv_sem=red_recv.at[number if buffer is gram0 else number + 1, offset + mine],
                    device_id=(base + lax.rem(mine + d, f) * stride,), device_id_type=MESH,
                ).wait_send()
            offset += f

    def send_loop(i, carry):
        halo_start(0, i)
        return carry

    lax.fori_loop(0, count, send_loop, 0)

    shifts = []
    for g in range(2):
        shift = jnp.float32(0.0)
        for s in range(table_ref.shape[0]):
            shift = shift + jnp.where(index_ref[g] == s, table_ref[s], 0.0)
        shifts.append(6.0 + shift)

    zero_rows = space.shape[1]
    for g in range(2):
        space[g, :, 0:LANES] = jnp.zeros((zero_rows, LANES), jnp.float32)
        space[g, :, cells + LANES : cells + 2 * LANES] = jnp.zeros((zero_rows, LANES), jnp.float32)
        if pad > k_rows:
            space[g, k_rows:pad, :] = jnp.zeros((pad - k_rows, space.shape[2]), jnp.float32)
    for side in range(2):
        @pl.when(jnp.logical_not(has[1 - side]))
        def _():
            halo_u[side] = jnp.zeros(halo_u.shape[1:], jnp.float32)
            for j in range(STEPS):
                halo_v[j, side] = jnp.zeros(halo_v.shape[2:], jnp.float32)

    lane = iota2((1, LANES), 1)

    def stencil(load, side0, side1, g, start):
        outer = start + LANES
        c = load(outer)
        near = load(outer - LANES) + load(outer + LANES)
        near = near + side0 + side1
        near = near + jnp.where(lane == 0, 0.0, pltpu.roll(c, 1, 1))
        near = near + jnp.where(lane == LANES - 1, 0.0, pltpu.roll(c, LANES - 1, 1))
        diag = med_ref[:, pl.ds(start, LANES)] + shifts[g]
        return diag * c - near

    def first_chunk(i, carry):
        halo_wait(0, i)
        out = []
        for g in range(2):
            for q in range(chunk // LANES):
                start = pl.multiple_of(i * chunk + q * LANES, LANES)
                here = pl.ds(start, LANES)
                applied = stencil(
                    lambda at: u_ref[g, :, pl.ds(pl.multiple_of(at, LANES), LANES)],
                    halo_u[0, g, :, here], halo_u[1, g, :, here], g, start,
                )
                there = pl.ds(pl.multiple_of(start + LANES, LANES), LANES)
                space[g, 0:k_rows, there] = applied
                space[g, pad : pad + block, there] = b_ref[g, :, here]
            outer = pl.ds(pl.multiple_of(i * chunk + LANES, LANES), chunk)
            rows = space[g, 0 : pad + block, outer]
            out.append(carry[g] + dot_t(rows, rows))
        return tuple(out)

    size = pad + block
    zero = jnp.zeros((size, size), jnp.float32)
    sums = lax.fori_loop(0, count, first_chunk, (zero, zero))
    filler = jnp.zeros((size, LANES), jnp.float32)
    for g in range(2):
        fin[g, 0:size, :] = filler
        fin[g, 0:size, 0:size] = sums[g]
    sums = reduce_sum(gram0, 0, [fin[g, 0:size, :] for g in range(2)])
    for g in range(2):
        fin[g, 0:size, :] = sums[g]
    linv = [z for _, z in factor_all([fin[g, 0:pad, 0:pad] for g in range(2)], k_rows)]
    proj_t = [dot_t(fin[g, pad:size, 0:pad], linv[g]) for g in range(2)]
    remaining = [fin[g, pad:size, pad:size] - dot_t(proj_t[g], proj_t[g]) for g in range(2)]
    first_factor = factor_all(remaining, block)
    for g in range(2):
        inv = first_factor[g][1]
        coef[g, :, 0:pad] = -dot(inv, dot(proj_t[g], linv[g]))
        coef[g, :, pad:size] = inv
        hbt[g, :, :] = jnp.zeros(hbt.shape[1:], jnp.float32)

    unit = eye(block)
    for j in range(1, STEPS + 1):
        known = pad + block * j

        def combine_chunk(i, carry):
            outer = pl.ds(pl.multiple_of(i * chunk + LANES, LANES), chunk)
            for g in range(2):
                space[g, known - block : known, outer] = dot(
                    coef[g, :, 0:known], space[g, 0:known, outer]
                )
            halo_start(j, i)
            return carry

        lax.fori_loop(0, count, combine_chunk, 0)

        def gram_chunk(i, carry):
            halo_wait(j, i)
            out = []
            for g in range(2):
                for q in range(chunk // LANES):
                    start = pl.multiple_of(i * chunk + q * LANES, LANES)
                    here = pl.ds(start, LANES)
                    space[g, known : known + block, pl.ds(pl.multiple_of(start + LANES, LANES), LANES)] = stencil(
                        lambda at: space[g, known - block : known, pl.ds(pl.multiple_of(at, LANES), LANES)],
                        halo_v[j - 1, 0, g, :, here], halo_v[j - 1, 1, g, :, here], g, start,
                    )
                outer = pl.ds(pl.multiple_of(i * chunk + LANES, LANES), chunk)
                rows = space[g, 0 : known + block, outer]
                out.append(carry[g] + dot_t(rows[known:, :], rows))
            return tuple(out)

        zero = jnp.zeros((block, known + block), jnp.float32)
        sums = lax.fori_loop(0, count, gram_chunk, (zero, zero))
        for g in range(2):
            fin[g, 0:block, 0 : known + block] = sums[g]
        sums = reduce_sum(gram, j - 1, [fin[g, 0:block, :] for g in range(2)])
        for g in range(2):
            fin[g, 0:block, :] = sums[g]
        et = [dot_t(fin[g, 0:block, 0:pad], linv[g]) for g in range(2)]
        ht = [fin[g, 0:block, pad:known] for g in range(2)]
        fresh = [
            fin[g, 0:block, known : known + block] - dot_t(et[g], et[g]) - dot_t(ht[g], ht[g])
            for g in range(2)
        ]
        parts = factor_all(fresh, block)
        for g in range(2):
            lt, inv = parts[g]
            coef[g, :, 0:pad] = -dot(inv, dot(et[g], linv[g]))
            coef[g, :, pad:known] = -dot(inv, ht[g])
            coef[g, :, known : known + block] = inv
            at = block * (j - 1)
            hbt[g, at : at + block, 0 : known - pad] = ht[g]
            hbt[g, at : at + block, known - pad : known - pad + block] = dot_t(unit, lt)
            ebt[g, at : at + block, :] = et[g]

    width = pad + block * (STEPS + 1)
    kry = block * STEPS
    normal, rights = [], []
    for g in range(2):
        h = hbt[g, :, 0 : kry + block]
        normal.append(dot_t(h, h))
        rights.append(dot(hbt[g, :, 0:block], first_factor[g][0]))
    ys = solve_all(normal, rights)
    for g in range(2):
        yt = dot_t(unit, ys[g])
        back[g, :, :] = dot(proj_t[g] - dot(yt, ebt[g, :, :]), linv[g])
        rest = -dot(yt, hbt[g, :, :])
        fin[g, 0:block, :] = rest
        fin[g, 0:block, 0:block] = fin[g, 0:block, 0:block] + dot_t(unit, first_factor[g][0])
        top = fin[g, 0:block, 0:kry]
        last = dot(fin[g, 0:block, kry : kry + block], coef[g, :, 0:width])
        fin[g, 0 : 2 * block, :] = jnp.zeros((2 * block, LANES), jnp.float32)
        fin[g, 0:block, pad : pad + kry] = yt
        fin[g, block : 2 * block, 0:width] = last
        fin[g, block : 2 * block, pad : pad + kry] = fin[g, block : 2 * block, pad : pad + kry] + top

    def final_chunk(i, carry):
        outer = pl.ds(pl.multiple_of(i * chunk + LANES, LANES), chunk)
        inner = pl.ds(pl.multiple_of(i * chunk, LANES), chunk)
        for g in range(2):
            both = dot(fin[g, 0 : 2 * block, 0:width], space[g, 0:width, outer])
            sol_ref[g, :, inner] = both[0:block] + dot(back[g, :, 0:k_rows], u_ref[g, :, outer])
            res_ref[g, :, inner] = both[block:]
        return carry

    lax.fori_loop(0, count, final_chunk, 0)

    for stage in range(STEPS + 1):
        def drain(i, carry):
            for side in range(2):
                @pl.when(has[side])
                def _():
                    halo_copy(stage, side, i).wait_send()
            return carry

        lax.fori_loop(0, count, drain, 0)
    reduce_drain(gram0, 0)
    for j in range(STEPS):
        reduce_drain(gram, j)


def split_count(n):
    out = []
    while n > 1:
        f = next(f for f in (8, 4, 2, n) if n % f == 0)
        out.append(f)
        n //= f
    return out


def solution(mesh):
    n = mesh.shape["grid"]
    factors = split_count(n)

    def on_device(right_sides, recycle, medium, shift_table, shift_index):
        block = right_sides.shape[0] // 2
        k_rows = recycle.shape[1]
        cells = right_sides.shape[2] * right_sides.shape[3]
        pad = -(-k_rows // block) * block
        tiles = cells // LANES
        chunk = LANES * next(t for t in (6, 4, 3, 2, 1) if tiles % t == 0)
        count = cells // chunk
        width = pad + block * (STEPS + 1)
        b = right_sides.reshape(2, block, cells)
        u = jnp.pad(recycle.reshape(2, k_rows, cells), ((0, 0), (0, 0), (LANES, LANES)))
        slots = sum(factors)
        vmem = pl.BlockSpec(memory_space=pltpu.VMEM)
        smem = pl.BlockSpec(memory_space=pltpu.SMEM)
        shape = jax.ShapeDtypeStruct((2, block, cells), jnp.float32)
        f32 = jnp.float32
        sol, res = pl.pallas_call(
            functools.partial(kernel, n, factors, chunk),
            out_shape=(shape, shape),
            in_specs=[vmem, vmem, vmem, smem, smem],
            out_specs=(vmem, vmem),
            scratch_shapes=[
                pltpu.VMEM((2, width, cells + 2 * LANES), f32),
                pltpu.VMEM((2, 2, k_rows, cells), f32),
                pltpu.VMEM((STEPS, 2, 2, block, cells), f32),
                pltpu.VMEM((1, slots, 2, pad + block, LANES), f32),
                pltpu.VMEM((STEPS, slots, 2, block, LANES), f32),
                pltpu.VMEM((2, block, LANES), f32),
                pltpu.VMEM((2, block * STEPS, LANES), f32),
                pltpu.VMEM((2, block * STEPS, pad), f32),
                pltpu.VMEM((2, pad + block, LANES), f32),
                pltpu.VMEM((2, block, pad), f32),
                pltpu.SemaphoreType.DMA((STEPS + 1, 2, count)),
                pltpu.SemaphoreType.DMA((STEPS + 1, 2, count)),
                pltpu.SemaphoreType.DMA((STEPS + 1, slots)),
                pltpu.SemaphoreType.DMA((STEPS + 1, slots)),
            ],
            compiler_params=pltpu.CompilerParams(
                collective_id=0, has_side_effects=True, vmem_limit_bytes=48 * 1024 * 1024
            ),
        )(u, b, medium.reshape(1, cells), shift_table, shift_index)
        return sol.reshape(right_sides.shape), res.reshape(right_sides.shape)

    rows = P(None, "grid", None, None)
    return jax.shard_map(
        on_device,
        mesh=mesh,
        in_specs=(rows, P(None, None, "grid", None, None), P("grid", None, None), P(), P()),
        out_specs=(rows, rows),
        check_vma=False,
    )
```

```python
import functools

import jax
import jax.numpy as jnp
from jax import lax
from jax.experimental import pallas as pl
from jax.experimental.pallas import tpu as pltpu
from jax.sharding import PartitionSpec as P

STEPS = 3
LANES = 128
MESH = pl.DeviceIdType.MESH
highest = lax.Precision.HIGHEST


def dot(left, right):
    return lax.dot_general(
        left, right, (((1,), (0,)), ((), ())), precision=highest, preferred_element_type=jnp.float32
    )


def dot_t(left, right):
    return lax.dot_general(
        left, right, (((1,), (1,)), ((), ())), precision=highest, preferred_element_type=jnp.float32
    )


def halves(x):
    high = x.astype(jnp.bfloat16)
    return high, (x - high.astype(jnp.float32)).astype(jnp.bfloat16)


def dot_three(left, right):
    a, b = halves(left), halves(right)
    one = lambda p, q: jnp.dot(p, q, preferred_element_type=jnp.float32)
    return one(a[0], b[0]) + (one(a[0], b[1]) + one(a[1], b[0]))


def iota2(shape, dim):
    return lax.broadcasted_iota(jnp.int32, shape, dim)


def eye(size):
    return jnp.where(iota2((size, size), 0) == iota2((size, size), 1), 1.0, 0.0)


def pair_step(arrays, k, first, second):
    c1, c2 = arrays[0][:, k : k + 1], arrays[0][:, k + 1 : k + 2]
    f1 = jnp.where(first, c1 * (1.0 / c1[k : k + 1]), 0.0)
    c2 = c2 - f1 * c2[k : k + 1]
    f2 = jnp.where(second, c2 * (1.0 / c2[k + 1 : k + 2]), 0.0)
    link = f1[k + 1 : k + 2]
    out = []
    for x in arrays:
        r1 = x[k : k + 1, :]
        r2 = x[k + 1 : k + 2, :] - link * r1
        out.append(x - f1 * r1 - f2 * r2)
    return tuple(out)


def factor_all(matrices, count):
    size = matrices[0].shape[0]
    rows = iota2((size, 1), 0)
    unit = jnp.where(rows < count, eye(size), 0.0)
    parts = [(m, unit) for m in matrices]
    for k in range(0, count, 2):
        parts = [pair_step(p, k, rows > k, rows > k + 1) for p in parts]
    upper = iota2((size, size), 1) >= iota2((size, size), 0)
    out = []
    for a, z in parts:
        pivots = jnp.sum(a * unit, axis=1, keepdims=True)
        root = jnp.where(rows < count, lax.rsqrt(jnp.where(rows < count, pivots, 1.0)), 0.0)
        out.append((jnp.where(upper, a * root, 0.0), z * root))
    return out


def solve_all(matrices, rights):
    size = matrices[0].shape[0]
    rows = iota2((size, 1), 0)
    unit = eye(size)
    parts = list(zip(matrices, rights))
    for k in range(0, size, 2):
        parts = [pair_step(p, k, rows != k, rows != k + 1) for p in parts]
    return [r / jnp.sum(a * unit, axis=1, keepdims=True) for a, r in parts]


def kernel(
    n, factors, chunk,
    u_ref, b_ref, med_ref, table_ref, index_ref, sol_ref, res_ref,
    space, halo_u, halo_v, gram0, gram, coef, hbt, ebt, fin, back,
    send_sem, recv_sem, red_send, red_recv,
):
    me = lax.axis_index("grid")
    k_rows = u_ref.shape[1]
    block = b_ref.shape[1]
    cells = b_ref.shape[2]
    count = cells // chunk
    pad = space.shape[1] - (STEPS + 1) * block
    left, right = me - 1, me + 1
    has = (me > 0, me < n - 1)

    barrier = pltpu.get_barrier_semaphore()
    peers = []
    stride = 1
    for f in factors:
        mine = lax.rem(me // stride, f)
        base = me - mine * stride
        peers.append((f, stride, mine, base))
        stride *= f
    total = 0
    for f, stride, mine, base in peers:
        for d in range(1, f):
            pl.semaphore_signal(
                barrier, inc=1, device_id=(base + lax.rem(mine + d, f) * stride,), device_id_type=MESH
            )
            total += 1
    for to in (lax.rem(me + n - 1, n), lax.rem(me + 1, n)):
        pl.semaphore_signal(barrier, inc=1, device_id=(to,), device_id_type=MESH)
    pl.semaphore_wait(barrier, total + 2)

    def halo_copy(stage, side, i):
        inner = pl.ds(pl.multiple_of(i * chunk, LANES), chunk)
        outer = pl.ds(pl.multiple_of(i * chunk + LANES, LANES), chunk)
        if stage == 0:
            src, dst = u_ref.at[:, :, outer], halo_u.at[side, :, :, inner]
        else:
            src = space.at[:, pl.ds(pad + block * (stage - 1), block), outer]
            dst = halo_v.at[stage - 1, side, :, :, inner]
        return pltpu.make_async_remote_copy(
            src_ref=src, dst_ref=dst,
            send_sem=send_sem.at[stage, side, i], recv_sem=recv_sem.at[stage, side, i],
            device_id=((left, right)[side],), device_id_type=MESH,
        )

    def halo_start(stage, i):
        for side in range(2):
            @pl.when(has[side])
            def _():
                halo_copy(stage, side, i).start()

    def halo_wait(stage, i):
        for side in range(2):
            @pl.when(has[1 - side])
            def _():
                halo_copy(stage, side, i).wait_recv()

    def reduce_sum(buffer, number, values):
        offset = 0
        for f, stride, mine, base in peers:
            own = offset + mine
            for g in range(len(values)):
                buffer[number, own, g, :, :] = values[g]
            for d in range(1, f):
                to = lax.rem(mine + d, f)
                pltpu.make_async_remote_copy(
                    src_ref=buffer.at[number, own], dst_ref=buffer.at[number, own],
                    send_sem=red_send.at[number if buffer is gram0 else number + 1, offset + d],
                    recv_sem=red_recv.at[number if buffer is gram0 else number + 1, own],
                    device_id=(base + to * stride,), device_id_type=MESH,
                ).start()
            for d in range(1, f):
                there = lax.rem(mine + d, f)
                origin = offset + there
                pltpu.make_async_remote_copy(
                    src_ref=buffer.at[number, origin], dst_ref=buffer.at[number, origin],
                    send_sem=red_send.at[number if buffer is gram0 else number + 1, offset + d],
                    recv_sem=red_recv.at[number if buffer is gram0 else number + 1, origin],
                    device_id=(base + there * stride,), device_id_type=MESH,
                ).wait_recv()
            held = len(values)
            values = []
            for g in range(held):
                value = buffer[number, offset, g, :, :]
                for s in range(1, f):
                    value = value + buffer[number, offset + s, g, :, :]
                values.append(value)
            offset += f
        return values

    def reduce_drain(buffer, number):
        offset = 0
        for f, stride, mine, base in peers:
            for d in range(1, f):
                pltpu.make_async_remote_copy(
                    src_ref=buffer.at[number, offset + mine], dst_ref=buffer.at[number, offset + mine],
                    send_sem=red_send.at[number if buffer is gram0 else number + 1, offset + d],
                    recv_sem=red_recv.at[number if buffer is gram0 else number + 1, offset + mine],
                    device_id=(base + lax.rem(mine + d, f) * stride,), device_id_type=MESH,
                ).wait_send()
            offset += f

    def send_loop(i, carry):
        halo_start(0, i)
        return carry

    lax.fori_loop(0, count, send_loop, 0)

    shifts = []
    for g in range(2):
        shift = jnp.float32(0.0)
        for s in range(table_ref.shape[0]):
            shift = shift + jnp.where(index_ref[g] == s, table_ref[s], 0.0)
        shifts.append(6.0 + shift)

    zero_rows = space.shape[1]
    for g in range(2):
        space[g, :, 0:LANES] = jnp.zeros((zero_rows, LANES), jnp.float32)
        space[g, :, cells + LANES : cells + 2 * LANES] = jnp.zeros((zero_rows, LANES), jnp.float32)
        if pad > k_rows:
            space[g, k_rows:pad, :] = jnp.zeros((pad - k_rows, space.shape[2]), jnp.float32)
    for side in range(2):
        @pl.when(jnp.logical_not(has[1 - side]))
        def _():
            halo_u[side] = jnp.zeros(halo_u.shape[1:], jnp.float32)
            for j in range(STEPS):
                halo_v[j, side] = jnp.zeros(halo_v.shape[2:], jnp.float32)

    lane = iota2((1, LANES), 1)

    def stencil(load, side0, side1, g, start):
        outer = start + LANES
        c = load(outer)
        near = load(outer - LANES) + load(outer + LANES)
        near = near + side0 + side1
        near = near + jnp.where(lane == 0, 0.0, pltpu.roll(c, 1, 1))
        near = near + jnp.where(lane == LANES - 1, 0.0, pltpu.roll(c, LANES - 1, 1))
        diag = med_ref[:, pl.ds(start, LANES)] + shifts[g]
        return diag * c - near

    def first_chunk(i, carry):
        halo_wait(0, i)
        out = []
        for g in range(2):
            for q in range(chunk // LANES):
                start = pl.multiple_of(i * chunk + q * LANES, LANES)
                here = pl.ds(start, LANES)
                applied = stencil(
                    lambda at: u_ref[g, :, pl.ds(pl.multiple_of(at, LANES), LANES)],
                    halo_u[0, g, :, here], halo_u[1, g, :, here], g, start,
                )
                there = pl.ds(pl.multiple_of(start + LANES, LANES), LANES)
                space[g, 0:k_rows, there] = applied
                space[g, pad : pad + block, there] = b_ref[g, :, here]
            outer = pl.ds(pl.multiple_of(i * chunk + LANES, LANES), chunk)
            rows = space[g, 0 : pad + block, outer]
            out.append(carry[g] + dot_t(rows, rows))
        return tuple(out)

    size = pad + block
    zero = jnp.zeros((size, size), jnp.float32)
    sums = lax.fori_loop(0, count, first_chunk, (zero, zero))
    half = LANES // 2
    fin[0, 0:size, :] = jnp.zeros((size, LANES), jnp.float32)
    for g in range(2):
        fin[0, 0:size, half * g : half * g + size] = sums[g]
    fin[0, 0:size, :] = reduce_sum(gram0, 0, [fin[0, 0:size, :]])[0]
    fin[1, 0:size, 0:size] = fin[0, 0:size, half : half + size]
    linv = [z for _, z in factor_all([fin[g, 0:pad, 0:pad] for g in range(2)], k_rows)]
    proj_t = [dot_t(fin[g, pad:size, 0:pad], linv[g]) for g in range(2)]
    remaining = [fin[g, pad:size, pad:size] - dot_t(proj_t[g], proj_t[g]) for g in range(2)]
    first_factor = factor_all(remaining, block)
    for g in range(2):
        inv = first_factor[g][1]
        coef[g, :, 0:pad] = -dot(inv, dot(proj_t[g], linv[g]))
        coef[g, :, pad:size] = inv
        hbt[g, :, :] = jnp.zeros(hbt.shape[1:], jnp.float32)

    unit = eye(block)
    for j in range(1, STEPS + 1):
        known = pad + block * j

        def combine_chunk(i, carry):
            outer = pl.ds(pl.multiple_of(i * chunk + LANES, LANES), chunk)
            for g in range(2):
                space[g, known - block : known, outer] = dot(
                    coef[g, :, 0:known], space[g, 0:known, outer]
                )
            halo_start(j, i)
            return carry

        lax.fori_loop(0, count, combine_chunk, 0)

        def gram_chunk(i, carry):
            halo_wait(j, i)
            out = []
            for g in range(2):
                for q in range(chunk // LANES):
                    start = pl.multiple_of(i * chunk + q * LANES, LANES)
                    here = pl.ds(start, LANES)
                    space[g, known : known + block, pl.ds(pl.multiple_of(start + LANES, LANES), LANES)] = stencil(
                        lambda at: space[g, known - block : known, pl.ds(pl.multiple_of(at, LANES), LANES)],
                        halo_v[j - 1, 0, g, :, here], halo_v[j - 1, 1, g, :, here], g, start,
                    )
                outer = pl.ds(pl.multiple_of(i * chunk + LANES, LANES), chunk)
                rows = space[g, 0 : known + block, outer]
                out.append(carry[g] + dot_t(rows[known:, :], rows))
            return tuple(out)

        zero = jnp.zeros((block, known + block), jnp.float32)
        sums = lax.fori_loop(0, count, gram_chunk, (zero, zero))
        for g in range(2):
            fin[g, 0:block, 0 : known + block] = sums[g]
        sums = reduce_sum(gram, j - 1, [fin[g, 0:block, :] for g in range(2)])
        for g in range(2):
            fin[g, 0:block, :] = sums[g]
        et = [dot_t(fin[g, 0:block, 0:pad], linv[g]) for g in range(2)]
        ht = [fin[g, 0:block, pad:known] for g in range(2)]
        fresh = [
            fin[g, 0:block, known : known + block] - dot_t(et[g], et[g]) - dot_t(ht[g], ht[g])
            for g in range(2)
        ]
        parts = factor_all(fresh, block)
        for g in range(2):
            lt, inv = parts[g]
            coef[g, :, 0:pad] = -dot(inv, dot(et[g], linv[g]))
            coef[g, :, pad:known] = -dot(inv, ht[g])
            coef[g, :, known : known + block] = inv
            at = block * (j - 1)
            hbt[g, at : at + block, 0 : known - pad] = ht[g]
            hbt[g, at : at + block, known - pad : known - pad + block] = dot_t(unit, lt)
            ebt[g, at : at + block, :] = et[g]

    width = pad + block * (STEPS + 1)
    kry = block * STEPS
    normal, rights = [], []
    for g in range(2):
        h = hbt[g, :, 0 : kry + block]
        normal.append(dot_t(h, h))
        rights.append(dot(hbt[g, :, 0:block], first_factor[g][0]))
    ys = solve_all(normal, rights)
    for g in range(2):
        yt = dot_t(unit, ys[g])
        back[g, :, :] = dot(proj_t[g] - dot(yt, ebt[g, :, :]), linv[g])
        rest = -dot(yt, hbt[g, :, :])
        fin[g, 0:block, :] = rest
        fin[g, 0:block, 0:block] = fin[g, 0:block, 0:block] + dot_t(unit, first_factor[g][0])
        top = fin[g, 0:block, 0:kry]
        last = dot(fin[g, 0:block, kry : kry + block], coef[g, :, 0:width])
        fin[g, 0 : 2 * block, :] = jnp.zeros((2 * block, LANES), jnp.float32)
        fin[g, 0:block, pad : pad + kry] = yt
        fin[g, block : 2 * block, 0:width] = last
        fin[g, block : 2 * block, pad : pad + kry] = fin[g, block : 2 * block, pad : pad + kry] + top

    def final_chunk(i, carry):
        outer = pl.ds(pl.multiple_of(i * chunk + LANES, LANES), chunk)
        inner = pl.ds(pl.multiple_of(i * chunk, LANES), chunk)
        for g in range(2):
            both = dot_three(fin[g, 0 : 2 * block, 0:width], space[g, 0:width, outer])
            sol_ref[g, :, inner] = both[0:block] + dot_three(back[g, :, 0:k_rows], u_ref[g, :, outer])
            res_ref[g, :, inner] = both[block:]
        return carry

    lax.fori_loop(0, count, final_chunk, 0)

    for stage in range(STEPS + 1):
        def drain(i, carry):
            for side in range(2):
                @pl.when(has[side])
                def _():
                    halo_copy(stage, side, i).wait_send()
            return carry

        lax.fori_loop(0, count, drain, 0)
    reduce_drain(gram0, 0)
    for j in range(STEPS):
        reduce_drain(gram, j)


def split_count(n):
    out = []
    while n > 1:
        f = next(f for f in (8, 4, 2, n) if n % f == 0)
        out.append(f)
        n //= f
    return out


def solution(mesh):
    n = mesh.shape["grid"]
    factors = split_count(n)

    def on_device(right_sides, recycle, medium, shift_table, shift_index):
        block = right_sides.shape[0] // 2
        k_rows = recycle.shape[1]
        cells = right_sides.shape[2] * right_sides.shape[3]
        pad = -(-k_rows // block) * block
        tiles = cells // LANES
        chunk = LANES * next(t for t in (6, 4, 3, 2, 1) if tiles % t == 0)
        count = cells // chunk
        width = pad + block * (STEPS + 1)
        b = right_sides.reshape(2, block, cells)
        u = jnp.pad(recycle.reshape(2, k_rows, cells), ((0, 0), (0, 0), (LANES, LANES)))
        slots = sum(factors)
        vmem = pl.BlockSpec(memory_space=pltpu.VMEM)
        smem = pl.BlockSpec(memory_space=pltpu.SMEM)
        shape = jax.ShapeDtypeStruct((2, block, cells), jnp.float32)
        f32 = jnp.float32
        sol, res = pl.pallas_call(
            functools.partial(kernel, n, factors, chunk),
            out_shape=(shape, shape),
            in_specs=[vmem, vmem, vmem, smem, smem],
            out_specs=(vmem, vmem),
            scratch_shapes=[
                pltpu.VMEM((2, width, cells + 2 * LANES), f32),
                pltpu.VMEM((2, 2, k_rows, cells), f32),
                pltpu.VMEM((STEPS, 2, 2, block, cells), f32),
                pltpu.VMEM((1, slots, 1, pad + block, LANES), f32),
                pltpu.VMEM((STEPS, slots, 2, block, LANES), f32),
                pltpu.VMEM((2, block, LANES), f32),
                pltpu.VMEM((2, block * STEPS, LANES), f32),
                pltpu.VMEM((2, block * STEPS, pad), f32),
                pltpu.VMEM((2, pad + block, LANES), f32),
                pltpu.VMEM((2, block, pad), f32),
                pltpu.SemaphoreType.DMA((STEPS + 1, 2, count)),
                pltpu.SemaphoreType.DMA((STEPS + 1, 2, count)),
                pltpu.SemaphoreType.DMA((STEPS + 1, slots)),
                pltpu.SemaphoreType.DMA((STEPS + 1, slots)),
            ],
            compiler_params=pltpu.CompilerParams(
                collective_id=0, has_side_effects=True, vmem_limit_bytes=48 * 1024 * 1024
            ),
        )(u, b, medium.reshape(1, cells), shift_table, shift_index)
        return sol.reshape(right_sides.shape), res.reshape(right_sides.shape)

    rows = P(None, "grid", None, None)
    return jax.shard_map(
        on_device,
        mesh=mesh,
        in_specs=(rows, P(None, None, "grid", None, None), P("grid", None, None), P(), P()),
        out_specs=(rows, rows),
        check_vma=False,
    )
```
